16 devices in a mesh: dp: 1, ep: 16 (over x, y, z, core).
Axes of the slice: x: 2, y: 2, z: 2, core: 2. Of those that a mesh axis runs over, the one named last changes fastest.
Arguments:
- x: bfloat16 [1, 16, 256, 1536], P('dp', 'ep')
- expert: int32 [1, 16, 256, 2], P('dp', 'ep')
- slot: int32 [1, 16, 256, 2], P('dp', 'ep')
- gate: float32 [1, 16, 256, 2], P('dp', 'ep')
- w_gate: bfloat16 [32, 1536, 9216], P('ep')
- w_up: bfloat16 [32, 1536, 9216], P('ep')
- w_down: bfloat16 [32, 9216, 1536], P('ep')
Outputs:
- y: bfloat16 [1, 16, 256, 1536], P('dp', 'ep')
All inputs are finite; a program needn't handle non-finite values.
Results may differ from the reference program's by a relative error of at most 0.009.
Values are sent between devices in bfloat16 or wider.
A program may use at most 2 GiB of HBM per device.

```python
import jax
import jax.numpy as jnp

MEMBERS = 16
TOKENS = 256
D = 1536
FF = 9216
TOP = 2
EXPERTS = 32
SLOTS = 5 * TOKENS * TOP // (4 * EXPERTS)


def setup_inputs(seed: int = 0, part: int = 0) -> dict:
    own, k1, k2, k3, k4, k5, k6 = jax.random.split(jax.random.key(seed), 7)
    kx, ke, kl, kg = jax.random.split(jax.random.fold_in(own, part), 4)
    devices = (1, MEMBERS)
    place = jax.random.permutation(kl, jnp.arange(EXPERTS, dtype=jnp.uint32))
    slow = ((EXPERTS + (9 * place) % EXPERTS) << ((9 * place) // EXPERTS)) // EXPERTS
    wait = (jax.random.bits(ke, (*devices, TOKENS, EXPERTS), jnp.uint32) >> 10) * slow
    expert = jnp.argsort(wait, axis=-1)[..., :TOP].astype(jnp.int32)
    chosen = jax.nn.one_hot(expert, EXPERTS, dtype=jnp.int32)
    in_line = jnp.cumsum(chosen.reshape(*devices, TOKENS * TOP, EXPERTS), axis=2) - 1
    slot = jnp.sum(in_line.reshape(chosen.shape) * chosen, axis=-1)

    def one(key, rows, columns):
        return (jax.random.normal(key, (rows, columns), jnp.float32) * rows**-0.5).astype(jnp.bfloat16)

    def weights(key, rows, columns):
        return jax.lax.map(lambda k: one(k, rows, columns), jax.random.split(key, EXPERTS))

    return {
        "x": jax.random.normal(kx, (*devices, TOKENS, D), jnp.float32).astype(jnp.bfloat16),
        "expert": expert,
        "slot": slot,
        "gate": jax.nn.softmax(jax.random.normal(kg, expert.shape, jnp.float32)),
        "w_gate": weights(k1, D, FF),
        "w_up": weights(k2, D, FF),
        "w_down": weights(k3, FF, D),
    }


def einsum(form, a, b):
    return jnp.einsum(form, a.astype(jnp.float32), b.astype(jnp.float32))


def reference(x, expert, slot, gate, w_gate, w_up, w_down):
    to_expert = jax.nn.one_hot(expert, EXPERTS, dtype=jnp.bfloat16)
    to_slot = jax.nn.one_hot(slot, SLOTS, dtype=jnp.bfloat16)
    weighted = to_expert * gate[..., None].astype(jnp.bfloat16)
    dispatch = einsum("abtke,abtkc->abtec", to_expert, to_slot).astype(jnp.bfloat16)
    combine = einsum("abtke,abtkc->abtec", weighted, to_slot).astype(jnp.bfloat16)
    z = einsum("abtec,abtd->aebcd", dispatch, x).astype(jnp.bfloat16)
    h = jax.nn.silu(einsum("aebcd,edf->aebcf", z, w_gate))
    h = (h * einsum("aebcd,edf->aebcf", z, w_up)).astype(jnp.bfloat16)
    out = einsum("aebcf,efd->aebcd", h, w_down).astype(jnp.bfloat16)
    y = einsum("abtec,aebcd->abtd", combine, out)
    return y.astype(jnp.bfloat16)
```

```python
import functools

import jax
import jax.numpy as jnp
from jax import lax
from jax.experimental import pallas as pl
from jax.experimental.pallas import tpu as pltpu
from jax.sharding import PartitionSpec as P

MESH = pl.DeviceIdType.MESH
F32, BF16 = jnp.float32, jnp.bfloat16

T, D, FF = 256, 1536, 9216
SLOTS = 20
GROUPS, PER = 2, 8
HALF = PER * SLOTS
ROWS = GROUPS * HALF
FC = 1536
NG = FF // FC
RG = 3
SUB = 256
NC = 512
NP = D // NC
KH = FF // 2
RD = 3
BLOCK = 80


def kernel(
    x_hbm, ex_hbm, sl_hbm, ga_hbm, wg, wu, wd, y_hbm,
    xb, exb, slb, gab, gbuf, ubuf, dbuf, h, z, snd, rcv, osnd, ret, cm, yacc, yb,
    insem, gsem, usem, dsem, ysem, ssem, rsem, ossem, orsem,
):
    me = lax.axis_index("ep")
    bits = [(me // w) % 2 for w in (8, 4, 2, 1)]

    def flips(g, jj):
        a, b = jj // 4, (jj // 2) % 2
        return a, b, (a + b + g) % 2, jj % 2

    def partner(g, jj):
        to = me
        for flip, bit, w in zip(flips(g, jj), bits, (8, 4, 2, 1)):
            if flip:
                to = to + (1 - 2 * bit) * w
        return to

    def g_copies(gi):
        e, i, s = gi // NG, gi % NG, gi % RG
        cols = pl.ds(pl.multiple_of(i * FC, FC), FC)
        return (
            pltpu.make_async_copy(wg.at[e, :, cols], gbuf.at[s], gsem.at[s]),
            pltpu.make_async_copy(wu.at[e, :, cols], ubuf.at[s], usem.at[s]),
        )

    def d_copy(di):
        e, p, half, s = di // (2 * NP), (di // 2) % NP, di % 2, di % RD
        return pltpu.make_async_copy(
            wd.at[e, pl.ds(pl.multiple_of(half * KH, KH), KH), pl.ds(pl.multiple_of(p * NC, NC), NC)],
            dbuf.at[s],
            dsem.at[s],
        )

    def dispatch_copy(e, g, jj):
        return pltpu.make_async_remote_copy(
            src_ref=snd.at[e, g, jj],
            dst_ref=rcv.at[e, g, jj],
            send_sem=ssem.at[e, g, jj],
            recv_sem=rsem.at[e, g, jj],
            device_id={"ep": partner(g, jj)} if isinstance(g, int) else {"ep": me},
            device_id_type=MESH,
        )

    def return_copy(e, p, g, jj):
        return pltpu.make_async_remote_copy(
            src_ref=osnd.at[e, p, g * PER + jj],
            dst_ref=ret.at[e, p, g * PER + jj],
            send_sem=ossem.at[e, p, g * PER + jj],
            recv_sem=orsem.at[e, p, g * PER + jj],
            device_id={"ep": partner(g, jj)},
            device_id_type=MESH,
        )

    partners = [(g, jj) for g in range(GROUPS) for jj in range(PER) if (g, jj) != (0, 0)]

    inputs = [
        pltpu.make_async_copy(a, b, insem.at[n])
        for n, (a, b) in enumerate(((ex_hbm, exb), (sl_hbm, slb), (ga_hbm, gab), (x_hbm, xb)))
    ]
    for c in inputs:
        c.start()
    for gi in range(RG):
        for c in g_copies(gi):
            c.start()
    for di in range(RD):
        d_copy(di).start()

    barrier = pltpu.get_barrier_semaphore()
    for g, jj in partners:
        pl.semaphore_signal(barrier, inc=1, device_id={"ep": partner(g, jj)}, device_id_type=MESH)
    for c in inputs:
        c.wait()

    key = jnp.where(slb[...] < SLOTS, exb[...] * 32 + slb[...], -1)
    key0 = jnp.broadcast_to(key[0:1], (16, T))
    key1 = jnp.broadcast_to(key[1:2], (16, T))
    row = lax.broadcasted_iota(jnp.int32, (16, T), 0)
    tile_of_row = lax.broadcasted_iota(jnp.int32, (16, 128), 0) // 4

    pl.semaphore_wait(barrier, len(partners))

    def dispatch(e, _):
        for g in range(GROUPS):
            marks = []
            for offset in (row, 16 + row % 4):
                for jj in range(PER):
                    want = offset + (2 * partner(g, jj) + e) * 32
                    hit = (key0 == want) | (key1 == want)
                    marks.append(jnp.where(hit, 1.0, 0.0).astype(BF16))
            marks = jnp.concatenate(marks, axis=0)
            for p in range(NP):
                v = jnp.dot(marks, xb[:, p * NC : (p + 1) * NC], preferred_element_type=F32)
                for jj in range(PER):
                    to = rcv if (g, jj) == (0, 0) else snd
                    for c in range(4):
                        part = v[jj * 16 : jj * 16 + 16, c * 128 : c * 128 + 128]
                        to[e, g, jj, p * BLOCK + c * 16 : p * BLOCK + c * 16 + 16, :] = part.astype(BF16)
                    rest = v[128 + jj * 16 : 128 + jj * 16 + 16]
                    part = rest[:, 0:128]
                    for c in range(1, 4):
                        part = jnp.where(tile_of_row == c, rest[:, c * 128 : c * 128 + 128], part)
                    to[e, g, jj, p * BLOCK + 64 : p * BLOCK + 80, :] = part.astype(BF16)
            for jj in range(PER):
                if (g, jj) != (0, 0):
                    dispatch_copy(e, g, jj).start()
        return 0

    lax.fori_loop(0, 2, dispatch, 0)

    def over_rows(v):
        v = jnp.transpose(jnp.broadcast_to(v, (128, T)))
        return jnp.concatenate([v, v], axis=1)

    keyf = key.astype(F32)
    k0, k1 = over_rows(keyf[0:1]), over_rows(keyf[1:2])
    g0, g1 = over_rows(gab[0:1]), over_rows(gab[1:2])
    lane = lax.broadcasted_iota(jnp.int32, (T, T), 1)
    j = lane // 16
    a, b = (j // 4) % 2, (j // 2) % 2
    flip = (a, b, (a + b + j // 8) % 2, j % 2)
    owner = sum(((f + bit) % 2) * w for f, bit, w in zip(flip, bits, (8, 4, 2, 1)))
    for e in range(2):
        for n, offset in enumerate((lane % 16, 16 + lane % 4)):
            want = ((2 * owner + e) * 32 + offset).astype(F32)
            v = jnp.where(k0 == want, g0, 0.0) + jnp.where(k1 == want, g1, 0.0)
            cm[e, n] = v.astype(BF16)

    def assemble(e, g):
        base = g * HALF
        for jj in range(PER):
            if jj == 0:

                @pl.when(g == 1)
                def _():
                    dispatch_copy(e, g, 0).wait_recv()
            else:
                dispatch_copy(e, g, jj).wait_recv()
        for jj in range(PER):
            for p in range(NP):
                for c in range(4):
                    z[pl.ds(pl.multiple_of(base + jj * 16, 16), 16), (p * 4 + c) * 128 : (p * 4 + c + 1) * 128] = rcv[
                        e, g, jj, p * BLOCK + c * 16 : p * BLOCK + c * 16 + 16, :
                    ]
        for quad in range(PER // 4):
            at = pl.ds(pl.multiple_of(base + 128 + quad * 16, 16), 16)
            for p in range(NP):
                rest = [rcv[e, g, quad * 4 + s, p * BLOCK + 64 : p * BLOCK + 80, :].astype(F32) for s in range(4)]
                for c in range(4):
                    v = jnp.concatenate([r[c * 4 : c * 4 + 4] for r in rest], axis=0)
                    z[at, (p * 4 + c) * 128 : (p * 4 + c + 1) * 128] = v.astype(BF16)

    def up(first, rows, i, s):
        at = pl.ds(first, rows)
        for n in range(FC // SUB):
            cols = slice(n * SUB, (n + 1) * SUB)
            gate = jnp.dot(z[at, :], gbuf[s, :, cols], preferred_element_type=F32)
            lift = jnp.dot(z[at, :], ubuf[s, :, cols], preferred_element_type=F32)
            v = gate / (1.0 + jnp.exp(-gate)) * lift
            h[at, pl.ds(pl.multiple_of(i * FC + n * SUB, SUB), SUB)] = v.astype(BF16)

    def early(g, _):
        assemble(0, g)

        def chunk(i, _):
            @pl.when(g == 0)
            def _():
                for c in g_copies(i):
                    c.wait()

            up(pl.multiple_of(g * HALF, 16), HALF, i, i)

            @pl.when(g == 1)
            def _():
                for c in g_copies(i + RG):
                    c.start()

            return 0

        return lax.fori_loop(0, RG, chunk, 0)

    lax.fori_loop(0, GROUPS, early, 0)

    def expert(e, _):
        @pl.when(e == 1)
        def _():
            def group(g, _):
                assemble(1, g)
                return 0

            lax.fori_loop(0, GROUPS, group, 0)

        def chunk(i, _):
            gi = e * NG + i
            for c in g_copies(gi):
                c.wait()
            up(0, ROWS, i, gi % RG)

            @pl.when(gi + RG < 2 * NG)
            def _():
                for c in g_copies(gi + RG):
                    c.start()

            return 0

        lax.fori_loop(RG - RG * e, NG, chunk, 0)

        def down(p, _):
            d0 = (e * NP + p) * 2
            d_copy(d0).wait()
            v = jnp.dot(h[:, 0:KH], dbuf[d0 % RD], preferred_element_type=F32)
            d_copy(d0 + 1).wait()
            v = jnp.dot(h[:, KH:FF], dbuf[(d0 + 1) % RD], preferred_element_type=F32) + v
            for g in range(GROUPS):
                for jj in range(PER):
                    to = ret if (g, jj) == (0, 0) else osnd
                    for c in range(4):
                        part = v[g * HALF + jj * 16 : g * HALF + jj * 16 + 16, c * 128 : c * 128 + 128]
                        to[e, p, g * PER + jj, c * 16 : c * 16 + 16, :] = part.astype(BF16)
                    rest = v[g * HALF + 128 + jj * 4 : g * HALF + 128 + jj * 4 + 4]
                    part = jnp.concatenate([rest[:, c * 128 : c * 128 + 128] for c in range(4)], axis=0)
                    to[e, p, g * PER + jj, 64:80, :] = part.astype(BF16)
            for g, jj in partners:
                return_copy(e, p, g, jj).start()
            for n in range(2):

                @pl.when(d0 + n + RD < 4 * NP)
                def _():
                    d_copy(d0 + n + RD).start()

            return 0

        return lax.fori_loop(0, NP, down, 0)

    lax.fori_loop(0, 2, expert, 0)

    tile_of = (lax.broadcasted_iota(jnp.int32, (T, 128), 0) // 4) % 4

    def total(n, _):
        e, p = n // NP, n % NP
        for g, jj in partners:
            return_copy(e, p, g, jj).wait_recv()
        main = jnp.concatenate(
            [ret[e, p, :, c * 16 : c * 16 + 16, :].reshape(T, 128) for c in range(4)], axis=1
        )
        rest = ret[e, p, :, 64:80, :].reshape(T, 128).astype(F32)
        rest = jnp.concatenate([jnp.where(tile_of == c, rest, 0.0).astype(BF16) for c in range(4)], axis=1)
        v = jnp.dot(cm[e, 0], main, preferred_element_type=F32) + jnp.dot(
            cm[e, 1], rest, preferred_element_type=F32
        )

        @pl.when(e == 0)
        def _():
            yacc[p] = v

        @pl.when(e == 1)
        def _():
            yb[p] = (yacc[p] + v).astype(BF16)
            pltpu.make_async_copy(
                yb.at[p], y_hbm.at[:, pl.ds(pl.multiple_of(p * NC, NC), NC)], ysem.at[p]
            ).start()

        return 0

    lax.fori_loop(0, 2 * NP, total, 0)

    for e in range(2):
        for g, jj in partners:
            dispatch_copy(e, g, jj).wait_send()
            for p in range(NP):
                return_copy(e, p, g, jj).wait_send()
    for p in range(NP):
        pltpu.make_async_copy(yb.at[p], y_hbm.at[:, p * NC : (p + 1) * NC], ysem.at[p]).wait()


def solution(mesh):
    dma = pltpu.SemaphoreType.DMA
    hbm = pl.BlockSpec(memory_space=pl.ANY)
    call = pl.pallas_call(
        kernel,
        out_shape=jax.ShapeDtypeStruct((T, D), BF16),
        in_specs=[hbm] * 7,
        out_specs=hbm,
        scratch_shapes=[
            pltpu.VMEM((T, D), BF16),
            pltpu.VMEM((2, T), jnp.int32),
            pltpu.VMEM((2, T), jnp.int32),
            pltpu.VMEM((2, T), F32),
            pltpu.VMEM((RG, D, FC), BF16),
            pltpu.VMEM((RG, D, FC), BF16),
            pltpu.VMEM((RD, KH, NC), BF16),
            pltpu.VMEM((ROWS, FF), BF16),
            pltpu.VMEM((ROWS, D), BF16),
            pltpu.VMEM((2, GROUPS, PER, NP * BLOCK, 128), BF16),
            pltpu.VMEM((2, GROUPS, PER, NP * BLOCK, 128), BF16),
            pltpu.VMEM((2, NP, GROUPS * PER, BLOCK, 128), BF16),
            pltpu.VMEM((2, NP, GROUPS * PER, BLOCK, 128), BF16),
            pltpu.VMEM((2, 2, T, T), BF16),
            pltpu.VMEM((NP, T, NC), F32),
            pltpu.VMEM((NP, T, NC), BF16),
            dma((4,)),
            dma((RG,)),
            dma((RG,)),
            dma((RD,)),
            dma((NP,)),
            dma((2, GROUPS, PER)),
            dma((2, GROUPS, PER)),
            dma((2, NP, GROUPS * PER)),
            dma((2, NP, GROUPS * PER)),
        ],
        compiler_params=pltpu.CompilerParams(
            collective_id=0, has_side_effects=True, vmem_limit_bytes=67043328
        ),
        name="moe",
    )

    def body(x, expert, slot, gate, w_gate, w_up, w_down):
        flat = [v.reshape(T, 2).T for v in (expert, slot, gate)]
        y = call(x.reshape(T, D), *flat, w_gate, w_up, w_down)
        return y.reshape(x.shape)

    tokens, experts = P("dp", "ep"), P("ep")
    return jax.shard_map(
        body, mesh=mesh, in_specs=(tokens,) * 4 + (experts,) * 3, out_specs=tokens, check_vma=False
    )
```

```python
import functools

import jax
import jax.numpy as jnp
from jax import lax
from jax.experimental import pallas as pl
from jax.experimental.pallas import tpu as pltpu
from jax.sharding import PartitionSpec as P

MESH = pl.DeviceIdType.MESH
F32, BF16 = jnp.float32, jnp.bfloat16

T, D, FF = 256, 1536, 9216
SLOTS = 20
GROUPS, PER = 2, 8
HALF = PER * SLOTS
ROWS = GROUPS * HALF
FC = 1536
NG = FF // FC
EARLY = 4
SUB = 256
NC = 512
NP = D // NC
KH = FF // 2
PAIRS = NG + NP
RING = 5
BLOCK = 80


def kernel(
    x_hbm, ex_hbm, sl_hbm, ga_hbm, wg, wu, wd, y_hbm,
    xb, exb, slb, gab, wbuf, h, z, snd, rcv, ret, cm, yacc,
    insem, wsem, ysem, ssem, rsem, ossem, orsem,
):
    me = lax.axis_index("ep")
    bits = [(me // w) % 2 for w in (8, 4, 2, 1)]

    def flips(g, jj):
        return tuple(int(jj // 2 == n) ^ g for n in (3, 2, 1)) + (jj % 2,)

    def partner(g, jj):
        to = me
        for flip, bit, w in zip(flips(g, jj), bits, (8, 4, 2, 1)):
            if flip:
                to = to + (1 - 2 * bit) * w
        return to

    def load(q, half):
        e, r, s = q // PAIRS, q % PAIRS, q % RING

        @pl.when(r < NG)
        def _():
            for b in range(FC // NC):
                cols = pl.ds(pl.multiple_of(r * FC + b * NC, NC), NC)
                pltpu.make_async_copy(
                    (wg, wu)[half].at[e, :, cols], wbuf.at[s, half, pl.ds(b * D, D)], wsem.at[s, half]
                ).start()

        @pl.when(r >= NG)
        def _():
            cols = pl.ds(pl.multiple_of((r - NG) * NC, NC), NC)
            pltpu.make_async_copy(
                wd.at[e, pl.ds(half * KH, KH), cols], wbuf.at[s, half], wsem.at[s, half]
            ).start()

    def load_after(q, half):
        @pl.when(q + RING < 2 * PAIRS)
        def _():
            load(q + RING, half)

    def loaded(q, half):
        s = q % RING
        pltpu.make_async_copy(
            wd.at[0, pl.ds(0, KH), pl.ds(0, NC)], wbuf.at[s, half], wsem.at[s, half]
        ).wait()

    def dispatch_copy(e, g, jj):
        return pltpu.make_async_remote_copy(
            src_ref=snd.at[e, g, jj],
            dst_ref=rcv.at[e, g, jj],
            send_sem=ssem.at[e, g],
            recv_sem=rsem.at[e, g],
            device_id={"ep": partner(g, jj)},
            device_id_type=MESH,
        )

    def dispatch_wait(e, g, sem):
        first = 1 if g == 0 else 0
        pltpu.make_async_copy(snd.at[e, g, first:PER], rcv.at[e, g, first:PER], sem.at[e, g]).wait()

    def return_copy(e, p, g, jj):
        return pltpu.make_async_remote_copy(
            src_ref=snd.at[e, g, jj, pl.ds(p * BLOCK, BLOCK)],
            dst_ref=ret.at[e, p, g * PER + jj],
            send_sem=ossem.at[e, p],
            recv_sem=orsem.at[e, p],
            device_id={"ep": partner(g, jj)},
            device_id_type=MESH,
        )

    def return_wait(e, p, sem):
        blocks = slice(1, GROUPS * PER)
        pltpu.make_async_copy(ret.at[e, p, blocks], ret.at[e, p, blocks], sem.at[e, p]).wait()

    partners = [(g, jj) for g in range(GROUPS) for jj in range(PER) if (g, jj) != (0, 0)]

    inputs = [
        pltpu.make_async_copy(a, b, insem.at[n])
        for n, (a, b) in enumerate(((ex_hbm, exb), (sl_hbm, slb), (ga_hbm, gab), (x_hbm, xb)))
    ]
    for c in inputs:
        c.start()

    barrier = pltpu.get_barrier_semaphore()
    for g, jj in partners:
        pl.semaphore_signal(barrier, inc=1, device_id={"ep": partner(g, jj)}, device_id_type=MESH)
    with jax.named_scope("in_wait"):
        for c in inputs:
            c.wait()
    for q in range(RING):
        for half in range(2):
            load(q, half)

    key = jnp.where(slb[...] < SLOTS, exb[...] * 32 + slb[...], -1)
    key0 = jnp.broadcast_to(key[0:1], (16, T))
    key1 = jnp.broadcast_to(key[1:2], (16, T))
    row = lax.broadcasted_iota(jnp.int32, (16, T), 0)
    tile_of_row = lax.broadcasted_iota(jnp.int32, (16, 128), 0) // 4

    with jax.named_scope("barrier"):
        pl.semaphore_wait(barrier, len(partners))

    def dispatch(e, _):
        for g in range(GROUPS):
            marks = []
            for offset in (row, 16 + row % 4):
                for jj in range(PER):
                    want = offset + (2 * partner(g, jj) + e) * 32
                    hit = (key0 == want) | (key1 == want)
                    marks.append(jnp.where(hit, 1.0, 0.0).astype(BF16))
            marks = jnp.concatenate(marks, axis=0)
            for p in range(NP):
                v = jnp.dot(marks, xb[:, p * NC : (p + 1) * NC], preferred_element_type=F32)
                for jj in range(PER):
                    to = rcv if (g, jj) == (0, 0) else snd
                    for c in range(4):
                        part = v[jj * 16 : jj * 16 + 16, c * 128 : c * 128 + 128]
                        to[e, g, jj, p * BLOCK + c * 16 : p * BLOCK + c * 16 + 16, :] = part.astype(BF16)
                    rest = v[128 + jj * 16 : 128 + jj * 16 + 16]
                    part = rest[:, 0:128]
                    for c in range(1, 4):
                        part = jnp.where(tile_of_row == c, rest[:, c * 128 : c * 128 + 128], part)
                    to[e, g, jj, p * BLOCK + 64 : p * BLOCK + 80, :] = part.astype(BF16)

            @pl.when(e == 0)
            def _():
                if g == 1:
                    dispatch_wait(0, 0, ssem)
                for jj in range(PER):
                    if (g, jj) != (0, 0):
                        dispatch_copy(0, g, jj).start()

        return 0

    with jax.named_scope("dispatch"):
        lax.fori_loop(0, 2, dispatch, 0)

    def over_rows(v):
        v = jnp.transpose(jnp.broadcast_to(v, (128, T)))
        return jnp.concatenate([v, v], axis=1)

    keyf = key.astype(F32)
    k0, k1 = over_rows(keyf[0:1]), over_rows(keyf[1:2])
    g0, g1 = over_rows(gab[0:1]), over_rows(gab[1:2])
    lane = lax.broadcasted_iota(jnp.int32, (T, T), 1)
    j = lane // 16
    flip = [(jnp.where((j // 2) % 4 == n, 1, 0) + j // 8) % 2 for n in (3, 2, 1)] + [j % 2]
    owner = sum(((f + bit) % 2) * w for f, bit, w in zip(flip, bits, (8, 4, 2, 1)))
    for e in range(2):
        for n, offset in enumerate((lane % 16, 16 + lane % 4)):
            want = ((2 * owner + e) * 32 + offset).astype(F32)
            v = jnp.where(k0 == want, g0, 0.0) + jnp.where(k1 == want, g1, 0.0)
            cm[e, n] = v.astype(BF16)

    def assemble(e, g):
        base = g * HALF
        with jax.named_scope("rows_wait"):
            for n in range(GROUPS):

                @pl.when(g == n)
                def _():
                    dispatch_wait(e, n, rsem)

        for jj in range(PER):
            for p in range(NP):
                for c in range(4):
                    z[pl.ds(pl.multiple_of(base + jj * 16, 16), 16), (p * 4 + c) * 128 : (p * 4 + c + 1) * 128] = rcv[
                        e, g, jj, p * BLOCK + c * 16 : p * BLOCK + c * 16 + 16, :
                    ]
        for quad in range(PER // 4):
            at = pl.ds(pl.multiple_of(base + 128 + quad * 16, 16), 16)
            for p in range(NP):
                rest = [rcv[e, g, quad * 4 + s, p * BLOCK + 64 : p * BLOCK + 80, :].astype(F32) for s in range(4)]
                for c in range(4):
                    v = jnp.concatenate([r[c * 4 : c * 4 + 4] for r in rest], axis=0)
                    z[at, (p * 4 + c) * 128 : (p * 4 + c + 1) * 128] = v.astype(BF16)

    def up(first, rows, i, s):
        at = pl.ds(first, rows)
        for n in range(FC // SUB):
            depth, cols = slice(n // 2 * D, n // 2 * D + D), slice(n % 2 * SUB, n % 2 * SUB + SUB)
            gate = jnp.dot(z[at, :], wbuf[s, 0, depth, cols], preferred_element_type=F32)
            lift = jnp.dot(z[at, :], wbuf[s, 1, depth, cols], preferred_element_type=F32)
            v = gate / (1.0 + jnp.exp(-gate)) * lift
            h[at, pl.ds(pl.multiple_of(i * FC + n * SUB, SUB), SUB)] = v.astype(BF16)

    def early(g, _):
        assemble(0, g)

        @pl.when(g == 1)
        def _():
            for to in partners:
                dispatch_copy(1, *to).start()

        def chunk(i, _):
            @pl.when(g == 0)
            def _():
                loaded(i, 0)
                loaded(i, 1)

            with jax.named_scope("up_half"):
                up(pl.multiple_of(g * HALF, 16), HALF, i, i)

            @pl.when(g == 1)
            def _():
                load(i + RING, 0)
                load(i + RING, 1)

            return 0

        return lax.fori_loop(0, EARLY, chunk, 0)

    lax.fori_loop(0, GROUPS, early, 0)

    def expert(e, _):
        @pl.when(e == 1)
        def _():
            def group(g, _):
                assemble(1, g)
                return 0

            lax.fori_loop(0, GROUPS, group, 0)

        def chunk(i, _):
            q = e * PAIRS + i
            with jax.named_scope("up_wait"):
                loaded(q, 0)
                loaded(q, 1)
            with jax.named_scope("up_all"):
                up(0, ROWS, i, q % RING)
            load_after(q, 0)
            load_after(q, 1)
            return 0

        lax.fori_loop(EARLY - EARLY * e, NG, chunk, 0)

        @pl.when(e == 0)
        def _():
            dispatch_wait(0, 1, ssem)

        @pl.when(e == 1)
        def _():
            for g in range(GROUPS):
                dispatch_wait(1, g, ssem)

        def back(e, p, g, v):
            for jj in range(PER):
                own = (g, jj) == (0, 0)
                to = ret.at[e, p, 0] if own else snd.at[e, g, jj, pl.ds(pl.multiple_of(p * BLOCK, BLOCK), BLOCK)]
                for c in range(4):
                    part = v[jj * 16 : jj * 16 + 16, c * 128 : c * 128 + 128]
                    to[c * 16 : c * 16 + 16, :] = part.astype(BF16)
                rest = v[128 + jj * 4 : 128 + jj * 4 + 4]
                part = jnp.concatenate([rest[:, c * 128 : c * 128 + 128] for c in range(4)], axis=0)
                to[64:80, :] = part.astype(BF16)
            for jj in range(PER):
                if (g, jj) != (0, 0):
                    return_copy(e, p, g, jj).start()

        @pl.when(e == 0)
        def _():
            def down(p, _):
                q = NG + p
                loaded(q, 0)
                with jax.named_scope("down0"):
                    v = jnp.dot(h[:, 0:KH], wbuf[q % RING, 0], preferred_element_type=F32)
                load_after(q, 0)
                loaded(q, 1)
                with jax.named_scope("down1"):
                    v = jnp.dot(h[:, KH:FF], wbuf[q % RING, 1], preferred_element_type=F32) + v
                for g in range(GROUPS):
                    back(0, p, g, v[g * HALF : (g + 1) * HALF])
                load_after(q, 1)
                return 0

            lax.fori_loop(0, NP, down, 0)

        @pl.when(e == 1)
        def _():
            def down(p, _):
                q = PAIRS + NG + p
                loaded(q, 0)
                for g in (1, 0):
                    rows = slice(g * HALF, (g + 1) * HALF)
                    with jax.named_scope("half0"):
                        v = jnp.dot(h[rows, 0:KH], wbuf[q % RING, 0], preferred_element_type=F32)
                    if g == 1:
                        loaded(q, 1)
                    with jax.named_scope("half1"):
                        v = jnp.dot(h[rows, KH:FF], wbuf[q % RING, 1], preferred_element_type=F32) + v
                    back(1, p, g, v)
                return 0

            lax.fori_loop(0, NP, down, 0)

        return 0

    lax.fori_loop(0, 2, expert, 0)

    tile_of = (lax.broadcasted_iota(jnp.int32, (T, 128), 0) // 4) % 4

    def total(n, _):
        e, p = n // NP, n % NP
        with jax.named_scope("total_wait"):
            return_wait(e, p, orsem)
        main = jnp.concatenate(
            [ret[e, p, :, c * 16 : c * 16 + 16, :].reshape(T, 128) for c in range(4)], axis=1
        )
        rest = ret[e, p, :, 64:80, :].reshape(T, 128).astype(F32)
        rest = jnp.concatenate([jnp.where(tile_of == c, rest, 0.0).astype(BF16) for c in range(4)], axis=1)
        v = jnp.dot(cm[e, 0], main, preferred_element_type=F32) + jnp.dot(
            cm[e, 1], rest, preferred_element_type=F32
        )

        @pl.when(e == 0)
        def _():
            yacc[p] = v

        @pl.when(e == 1)
        def _():
            cols = pl.ds(pl.multiple_of(p * NC, NC), NC)
            xb[:, cols] = (yacc[p] + v).astype(BF16)
            pltpu.make_async_copy(xb.at[:, cols], y_hbm.at[:, cols], ysem.at[p]).start()

        return 0

    lax.fori_loop(0, 2 * NP, total, 0)

    with jax.named_scope("drain"):
        for e in range(2):
            for p in range(NP):
                return_wait(e, p, ossem)
        for p in range(NP):
            cols = slice(p * NC, (p + 1) * NC)
            pltpu.make_async_copy(xb.at[:, cols], y_hbm.at[:, cols], ysem.at[p]).wait()


def solution(mesh):
    dma = pltpu.SemaphoreType.DMA
    hbm = pl.BlockSpec(memory_space=pl.ANY)
    call = pl.pallas_call(
        kernel,
        out_shape=jax.ShapeDtypeStruct((T, D), BF16),
        in_specs=[hbm] * 7,
        out_specs=hbm,
        scratch_shapes=[
            pltpu.VMEM((T, D), BF16),
            pltpu.VMEM((2, T), jnp.int32),
            pltpu.VMEM((2, T), jnp.int32),
            pltpu.VMEM((2, T), F32),
            pltpu.VMEM((RING, 2, KH, NC), BF16),
            pltpu.VMEM((ROWS, FF), BF16),
            pltpu.VMEM((ROWS, D), BF16),
            pltpu.VMEM((2, GROUPS, PER, NP * BLOCK, 128), BF16),
            pltpu.VMEM((2, GROUPS, PER, NP * BLOCK, 128), BF16),
            pltpu.VMEM((2, NP, GROUPS * PER, BLOCK, 128), BF16),
            pltpu.VMEM((2, 2, T, T), BF16),
            pltpu.VMEM((NP, T, NC), F32),
            dma((4,)),
            dma((RING, 2)),
            dma((NP,)),
            dma((2, GROUPS)),
            dma((2, GROUPS)),
            dma((2, NP)),
            dma((2, NP)),
        ],
        compiler_params=pltpu.CompilerParams(
            collective_id=0, has_side_effects=True, vmem_limit_bytes=67043328
        ),
        name="moe",
    )

    def body(x, expert, slot, gate, w_gate, w_up, w_down):
        flat = [v.reshape(T, 2).T for v in (expert, slot, gate)]
        y = call(x.reshape(T, D), *flat, w_gate, w_up, w_down)
        return y.reshape(x.shape)

    tokens, experts = P("dp", "ep"), P("ep")
    return jax.shard_map(
        body, mesh=mesh, in_specs=(tokens,) * 4 + (experts,) * 3, out_specs=tokens, check_vma=False
    )
```
